32 devices in a mesh: dp: 8 (over z, x), fsdp: 4 (over y, core).
Axes of the slice: x: 2, y: 2, z: 4, core: 2. Of those that a mesh axis runs over, the one named last changes fastest.
Arguments:
- text_states: bfloat16 [24, 64, 4096], P('dp', None, 'fsdp'), may hold values from -6 to 6
- cotangent: bfloat16 [24, 64, 4096], P('dp', None, 'fsdp'), may hold values from -6 to 6
- norm_gain: float32 [4096], replicated, may hold values from 0.5 to 120
- norm_bias: float32 [4096], replicated, may hold values from -3 to 3
- branch_gate: float32 [1], replicated, may hold values from 0.4 to 1.2
- query_weight: bfloat16 [4096, 16, 128], P(None, 'fsdp'), may hold values from -0.09375 to 0.09375
- latent_weight: bfloat16 [4096, 16, 256], P(None, 'fsdp'), may hold values from -0.09375 to 0.09375
- output_weight: bfloat16 [16, 128, 4096], P('fsdp'), may hold values from -0.125 to 0.125
- latents: bfloat16 [72, 64, 4096], P('dp'), may hold values from -6 to 6
- media_refs: int32 [24, 5], replicated, may hold values from -1 to 71, as said below
- media_pos: int32 [24, 64], P('dp'), may hold values from -1 to 4, as said below
- owner_map: int32 [72], replicated, may hold values from 0 to 71, as said below
Outputs:
- layer_out: bfloat16 [24, 64, 4096], P('dp', None, 'fsdp')
- out_grad: float32 [16, 128, 4096], P('fsdp', None, 'dp')
The draws below stay inside these ranges and needn't reach their ends.
Inputs may be any that keep to these rules, and one draw needn't show every extreme that they name: `media_refs`: row s holds the ids of sequence s's images in its first 1 to 5 entries, the rest are -1; every image id stands in exactly one row. A permutation: image i's latents are storage row owner_map[i], held by data shard owner_map[i] // 9. The images of one data shard's sequences lie on at most 2 storage rows of any one data shard, and some data shard reaches 2. `media_pos`: for each token, the number of its sequence's images placed at or before it, minus one; images take increasing positions in the window, each image has tokens, and a slot named is always filled in media_refs.
All inputs are finite; a program needn't handle non-finite values.
Results may differ from the reference program's by a relative error of at most 0.039.
The reference program's roundings to bfloat16 on the way count: a program that leaves them out, or rounds other values in their place, can miss the bound.
Values may be sent and summed in bfloat16 or wider, within the bound.
No kernel may reach another device: no remote copies, remote signals or barrier semaphores. Data moves between devices by JAX's collectives and lax.ppermute only.
A program may use at most 128 MiB of HBM per device.

```python
import jax
import jax.numpy as jnp
from jax import lax

D = 4096
HEADS = 16
HD = 128
LAT = 64
MAXIMG = 5
SEQ_DP = 3
WIN = 64
SEQS = 24
IMG_DP = 9
IMAGES = 72


def media_plan(key):
    count_key = jax.random.fold_in(key, 101)
    order_key = jax.random.fold_in(key, 102)
    owner_key = jax.random.fold_in(key, 103)
    shift_key = jax.random.fold_in(key, 104)
    turn_key = jax.random.fold_in(key, 105)
    place_key = jax.random.fold_in(key, 106)
    start_key = jax.random.fold_in(key, 107)
    groups = SEQS // SEQ_DP
    half_count = SEQS // 2
    first_half = jax.random.randint(count_key, (half_count,), 1, MAXIMG + 1)
    first_half = jnp.where(jnp.arange(half_count) < SEQ_DP, MAXIMG, first_half)
    counts = jnp.concatenate([first_half, MAXIMG + 1 - first_half]).astype(jnp.int32)
    offsets = jnp.cumsum(counts) - counts
    entry = jnp.arange(MAXIMG, dtype=jnp.int32)
    order_slot = offsets[:, None] + entry[None, :]
    live = entry[None, :] < counts[:, None]
    image_order = jax.random.permutation(order_key, IMAGES).astype(jnp.int32)
    refs = jnp.where(live, image_order[jnp.minimum(order_slot, IMAGES - 1)], -1).astype(jnp.int32)
    owner_order = jax.random.permutation(owner_key, groups).astype(jnp.int32)
    shift_amount = jax.random.randint(shift_key, (), 0, groups)
    turns = jax.random.randint(turn_key, (groups,), 0, IMG_DP)
    ranked = jnp.arange(IMAGES, dtype=jnp.int32) + shift_amount
    residue = ranked % groups
    within = (ranked // groups + turns[residue]) % IMG_DP
    storage = owner_order[residue] * IMG_DP + within
    owners = jnp.zeros((IMAGES,), jnp.int32).at[image_order].set(storage.astype(jnp.int32))
    first_place = jax.random.randint(start_key, (SEQS, 1), 0, max(WIN // 8, 1))
    gaps = jax.random.randint(place_key, (SEQS, MAXIMG - 1), 1, max(WIN // MAXIMG, 2))
    places = jnp.concatenate([first_place, first_place + jnp.cumsum(gaps, axis=1)], axis=1)
    token_index = jnp.arange(WIN, dtype=jnp.int32)
    seen = (places[:, None, :] <= token_index[None, :, None]) & live[:, None, :]
    positions = (jnp.sum(seen.astype(jnp.int32), axis=-1) - 1).astype(jnp.int32)
    return (refs, owners, positions)


def draw_media_refs(key, part):
    return media_plan(key)[0]


def draw_owner_map(key, part):
    return media_plan(key)[1]


def draw_media_pos(key, part):
    return media_plan(key)[2]


def draw_norm_gain(key, part):
    spread = jax.random.truncated_normal(jax.random.fold_in(key, 302), -5.0, 5.0, (D,), jnp.float32)
    return (1.0 + 0.1 * spread).astype(jnp.float32)


def raised(drawn, key, source, target, blocks, factor):
    def block_of(dim):
        return (jnp.arange(drawn.shape[dim]) // (drawn.shape[dim] // blocks)).reshape((-1,) + (1,) * (drawn.ndim - 1 - dim))

    near = jax.random.permutation(key, blocks)[block_of(target)]
    far = (block_of(target) + blocks // 2) % blocks
    return jnp.where((block_of(source) == near) | (block_of(source) == far), factor * drawn, drawn)


def shard_levels(own_key, extent, split, smallest, high):
    factor_of, own = 1.0, jax.random.fold_in(own_key, 6)
    for axis_at, blocks in split:
        draws = jnp.exp(jax.random.uniform(jax.random.fold_in(own, axis_at), (blocks,), jnp.float32, smallest / len(split), high / len(split)))
        factor_of = factor_of * jnp.repeat(draws, extent[axis_at] // blocks).reshape([-1 if axis == axis_at else 1 for axis in range(len(extent))])
    return factor_of


def scatter_about(own_key, shape, scale, reach, pieces=(), held_as=jnp.bfloat16):
    level = shard_levels(own_key, shape, pieces, -0.22, 0.18) if pieces else 1.0
    array = jax.random.normal(own_key, shape, jnp.float32) * scale * level
    return jnp.minimum(jnp.maximum(array, -reach), reach).astype(held_as)


def heavy_noise(key, extent, scale, most, shards, heavy, held_as=jnp.bfloat16):
    drawn = scale * jax.random.normal(key, extent, jnp.float32)
    if shards:
        drawn = drawn * shard_levels(key, extent, shards, -0.22, 0.18)
    return jnp.clip(raised(drawn, jax.random.fold_in(key, 3), *heavy), -most, most).astype(held_as)


def setup_inputs(seed: int = 0) -> dict:
    streams_of = jax.random.split(jax.random.key(seed), 13)
    text_states = scatter_about(streams_of[0], (SEQS, WIN, D), 1.0, 6.0, ((0, 8), (2, 4)))
    cotangent = heavy_noise(streams_of[1], (SEQS, WIN, D), 1.0, 6.0, ((0, 8), (2, 4)), (0, 2, 8, 2.0))
    norm_gain = draw_norm_gain(jax.random.fold_in(streams_of[12], 71), 0)
    norm_bias = scatter_about(streams_of[3], (D,), 0.5, 3.0, (), jnp.float32)
    branch_gate = jnp.clip(jax.random.uniform(streams_of[4], (1,), jnp.float32, 0.4, 1.2), 0.4, 1.2)
    query_weight = scatter_about(streams_of[5], (D, HEADS, HD), D ** -0.5, 0.09375, ((1, 4),))
    latent_weight = scatter_about(streams_of[6], (D, HEADS, 2 * HD), D ** -0.5, 0.09375, ((1, 4),))
    output_weight = scatter_about(streams_of[7], (HEADS, HD, D), (HEADS * HD) ** -0.5, 0.125, ((0, 4),))
    latents = scatter_about(streams_of[8], (IMAGES, LAT, D), 1.0, 6.0, ((0, 8),))
    media_refs = draw_media_refs(jax.random.fold_in(streams_of[12], 71), 0)
    media_pos = draw_media_pos(jax.random.fold_in(streams_of[12], 71), 0)
    owner_map = draw_owner_map(jax.random.fold_in(streams_of[12], 71), 0)
    return {"text_states": text_states, "cotangent": cotangent, "norm_gain": norm_gain, "norm_bias": norm_bias, "branch_gate": branch_gate, "query_weight": query_weight, "latent_weight": latent_weight, "output_weight": output_weight, "latents": latents, "media_refs": media_refs, "media_pos": media_pos, "owner_map": owner_map}


def reference(text_states, cotangent, norm_gain, norm_bias, branch_gate, query_weight, latent_weight, output_weight, latents, media_refs, media_pos, owner_map):
    tokens = SEQS * WIN
    as_float = text_states.astype(jnp.float32).reshape(tokens, D)
    row_mean = lax.optimization_barrier(jnp.mean(as_float, axis=-1, keepdims=True))
    centered = as_float - row_mean
    variance = lax.optimization_barrier(jnp.mean(centered * centered, axis=-1, keepdims=True))
    normed = (centered * lax.rsqrt(variance + 1e-05) * norm_gain + norm_bias).astype(jnp.bfloat16)
    queries = jnp.dot(normed, query_weight.reshape(D, HEADS * HD), preferred_element_type=jnp.float32)
    queries = (queries * HD ** (-0.5)).astype(jnp.bfloat16).reshape(SEQS, WIN, HEADS, HD)
    pairs = jnp.dot(latents.reshape(IMAGES * LAT, D), latent_weight.reshape(D, HEADS * 2 * HD), preferred_element_type=jnp.float32)
    pairs = pairs.astype(jnp.bfloat16).reshape(IMAGES, LAT, HEADS, 2 * HD)
    ref_storage = owner_map[jnp.maximum(media_refs, 0)].astype(jnp.int32)
    column_image = jnp.arange(MAXIMG * LAT, dtype=jnp.int32) // LAT

    def one_sequence(packed):
        query_block, position, storage = packed
        block = pairs[storage].reshape(MAXIMG * LAT, HEADS, 2 * HD)
        key_part = block[:, :, :HD].astype(jnp.float32)
        value_part = block[:, :, HD:].astype(jnp.float32)
        scores = jnp.einsum('the,mhe->htm', query_block.astype(jnp.float32), key_part)
        allowed = position[:, None] == column_image[None, :]
        scores = jnp.where(allowed[None], scores, -1e+30)
        row_max = lax.optimization_barrier(jnp.max(scores, axis=-1, keepdims=True))
        weights = jnp.exp(scores - row_max)
        softmaxed = (weights / lax.optimization_barrier(jnp.sum(weights, axis=-1, keepdims=True))).astype(jnp.bfloat16)
        context = jnp.einsum('htm,mhe->the', softmaxed.astype(jnp.float32), value_part)
        context = jnp.where(position[:, None, None] >= 0, context, 0.0)
        return context.astype(jnp.bfloat16)
    context = lax.map(one_sequence, (queries, media_pos, ref_storage))
    context_rows = context.reshape(tokens, HEADS * HD)
    update = jnp.dot(context_rows, output_weight.reshape(HEADS * HD, D), preferred_element_type=jnp.float32)
    gate_scale = jnp.tanh(branch_gate[0])
    layer_out = (as_float + gate_scale * update).reshape(SEQS, WIN, D).astype(jnp.bfloat16)
    gradient = jnp.dot(context_rows.T, cotangent.reshape(tokens, D), preferred_element_type=jnp.float32)
    out_grad = (gate_scale * gradient).reshape(HEADS, HD, D)
    return (layer_out, out_grad)
```

```python
import functools

import jax
import jax.numpy as jnp
from jax import lax
from jax.experimental import pallas as pl
from jax.experimental.pallas import tpu as pltpu
from jax.sharding import PartitionSpec as P

EPSILON = 1e-05
F32 = jnp.float32
BF16 = jnp.bfloat16


def swap(value, axis, offset):
    size = lax.axis_size(axis)
    return lax.ppermute(value, axis, [(i, i ^ offset) for i in range(size)])


def layer_norm(row_values, norm_gain, norm_bias):
    as_float = row_values.astype(F32)
    row_mean = jnp.mean(as_float, axis=-1, keepdims=True)
    centered = as_float - row_mean
    variance = jnp.mean(centered * centered, axis=-1, keepdims=True)
    return (centered * lax.rsqrt(variance + EPSILON) * norm_gain + norm_bias).astype(BF16)


def gather_blocks(value, axis):
    size = lax.axis_size(axis)
    blocks = {0: value}
    step = size // 2
    while step:
        for offset in list(blocks):
            blocks[offset | step] = swap(blocks[offset], axis, step)
        step //= 2
    return [blocks[j] for j in range(size)]


def dispatch_kernel(groups, per_group, capacity, images_local, chunks, me_ref, refs_ref, owner_ref, pairs_ref, *rest):
    outs, picked = rest[:-1], rest[-1]
    me = me_ref[0]
    for index in range(groups * capacity):
        picked[index] = 0

    def per_target(offset, carry):
        target = me ^ offset

        def per_ref(position, count):
            image = refs_ref[target * per_group + position]
            storage = owner_ref[jnp.maximum(image, 0)]
            hit = (image >= 0) & (storage // images_local == me)

            @pl.when(hit)
            def _():
                picked[offset * capacity + jnp.minimum(count, capacity - 1)] = storage % images_local

            return count + hit.astype(jnp.int32)

        lax.fori_loop(0, per_group, per_ref, 0)
        return carry

    lax.fori_loop(0, groups, per_target, 0)
    heads = outs[0].shape[0]
    for offset in range(groups):
        for slot in range(capacity):
            index = picked[offset * capacity + slot]
            for chunk in range(chunks):
                out = outs[chunk * groups + offset]
                for head in range(heads):
                    out[head, slot] = pairs_ref[chunk * heads + head, index]


def dispatch(me, media_refs, owner_map, pairs, groups, capacity, chunks):
    heads, images_local, latent_rows, width = pairs.shape
    per_group = media_refs.size // groups
    shape = (heads // chunks, capacity, latent_rows, width)
    smem = pl.BlockSpec(memory_space=pltpu.SMEM)
    vmem = pl.BlockSpec(memory_space=pltpu.VMEM)
    return pl.pallas_call(
        functools.partial(dispatch_kernel, groups, per_group, capacity, images_local, chunks),
        out_shape=[jax.ShapeDtypeStruct(shape, BF16)] * (groups * chunks),
        in_specs=[smem, smem, smem, vmem],
        out_specs=[vmem] * (groups * chunks),
        scratch_shapes=[pltpu.SMEM((groups * capacity,), jnp.int32)],
        name="dispatch",
    )(me.reshape(1), media_refs.reshape(-1), owner_map, pairs)


def attend_kernel(groups, latent_rows, head_size, slot_ref, query_ref, *rest):
    bufs, out = rest[:-1], rest[-1]
    slot = slot_ref[...]
    heads = bufs[0].shape[0]
    per_source = bufs[0].shape[1]
    columns = lax.broadcasted_iota(jnp.int32, (slot.shape[0], groups * per_source), 1) // latent_rows
    allowed = columns == slot
    for head in range(heads):
        lanes = slice(head * head_size, (head + 1) * head_size)
        query = query_ref[:, lanes]
        scores = jnp.concatenate(
            [
                lax.dot_general(query, buf[head, :, :head_size], (((1,), (1,)), ((), ())), preferred_element_type=F32)
                for buf in bufs
            ],
            axis=1,
        )
        scores = jnp.where(allowed, scores, -1e30)
        weights = jnp.exp(scores - jnp.max(scores, axis=-1, keepdims=True))
        probs = (weights / jnp.sum(weights, axis=-1, keepdims=True)).astype(BF16)
        values = jnp.concatenate([buf[head, :, head_size:] for buf in bufs], axis=0)
        context = jnp.dot(probs, values, preferred_element_type=F32)
        out[:, lanes] = jnp.where(slot >= 0, context, 0.0).astype(BF16)


def attend(slots, queries, buffers, chunk, head_size):
    groups = len(buffers)
    heads, capacity, latent_rows, width = buffers[0].shape
    tokens = queries.shape[0]
    lanes = heads * head_size
    buffers = [b.reshape(heads, capacity * latent_rows, width) for b in buffers]
    whole = pl.BlockSpec((heads, capacity * latent_rows, width), lambda i: (0, 0, 0))
    return pl.pallas_call(
        functools.partial(attend_kernel, groups, latent_rows, head_size),
        grid=(1,),
        out_shape=jax.ShapeDtypeStruct((tokens, lanes), BF16),
        in_specs=[
            pl.BlockSpec((tokens, 1), lambda i: (0, 0)),
            pl.BlockSpec((tokens, lanes), lambda i: (0, chunk)),
        ]
        + [whole] * groups,
        out_specs=pl.BlockSpec((tokens, lanes), lambda i: (0, 0)),
        name="attend",
    )(slots, queries, *buffers)


def grad_kernel(groups, aliased, gate_ref, cot_ref, *rest):
    contexts = rest[:groups]
    out = rest[-1]
    rows = jnp.concatenate([c[...] for c in contexts], axis=0)
    grad = lax.dot_general(rows, cot_ref[...], (((0,), (0,)), ((), ())), preferred_element_type=F32)
    out[...] = gate_ref[0] * grad


def grad_part(gate, cot_rows, contexts, chunk, chunks, previous):
    groups = len(contexts)
    tokens, lanes = contexts[0].shape
    cols = cot_rows.shape[1]
    whole = pl.BlockSpec((tokens, lanes), lambda i: (0, 0))
    in_specs = [
        pl.BlockSpec(memory_space=pltpu.SMEM),
        pl.BlockSpec(cot_rows.shape, lambda i: (0, 0)),
    ] + [whole] * groups
    operands = [gate, cot_rows, *contexts]
    aliases = {}
    if previous is not None:
        in_specs.append(pl.BlockSpec(memory_space=pl.ANY))
        aliases = {len(operands): 0}
        operands.append(previous)
    return pl.pallas_call(
        functools.partial(grad_kernel, groups, previous is not None),
        grid=(1,),
        out_shape=jax.ShapeDtypeStruct((chunks * lanes, cols), F32),
        in_specs=in_specs,
        out_specs=pl.BlockSpec((lanes, cols), lambda i: (chunk, 0)),
        input_output_aliases=aliases,
        name="grad",
    )(*operands)


def body(
    text_states,
    cotangent,
    norm_gain,
    norm_bias,
    branch_gate,
    query_weight,
    latent_weight,
    output_weight,
    latents,
    media_refs,
    media_pos,
    owner_map,
):
    seq_local, window, feat_local = text_states.shape
    model_width = query_weight.shape[0]
    head_local, head_size = query_weight.shape[1], query_weight.shape[2]
    img_local, latent_rows = latents.shape[0], latents.shape[1]
    groups, shards = lax.axis_size("dp"), lax.axis_size("fsdp")
    me, shard = lax.axis_index("dp"), lax.axis_index("fsdp")
    per_sequence = media_refs.shape[1]
    slot_count = media_refs.shape[0] * per_sequence // groups
    capacity = (slot_count + groups - 1) // groups
    tokens = seq_local * window
    chunks = 2 if head_local % 2 == 0 else 1
    gate_scale = jnp.tanh(branch_gate)

    pairs = jnp.einsum(
        "nd,dhe->hne", latents.reshape(img_local * latent_rows, model_width), latent_weight, preferred_element_type=F32
    ).astype(BF16)
    pairs = pairs.reshape(head_local, img_local, latent_rows, 2 * head_size)
    outgoing = dispatch(me, media_refs, owner_map, pairs, groups, capacity, chunks)
    arrived = []
    for chunk in range(chunks):
        part = outgoing[chunk * groups : (chunk + 1) * groups]
        arrived.append([part[0]] + [swap(part[d], "dp", d) for d in range(1, groups)])

    text_blocks = gather_blocks(text_states.reshape(tokens, feat_local), "fsdp")
    text_rows = jnp.zeros((tokens, model_width), BF16)
    for j, block in enumerate(text_blocks):
        text_rows = lax.dynamic_update_slice(text_rows, block, (0, (shard ^ j) * feat_local))
    normed = layer_norm(text_rows, norm_gain, norm_bias)
    queries = jnp.dot(normed, query_weight.reshape(model_width, head_local * head_size), preferred_element_type=F32)
    queries = (queries * head_size ** (-0.5)).astype(BF16)

    own_refs = lax.dynamic_slice_in_dim(media_refs, me * seq_local, seq_local, 0).reshape(slot_count)
    present = own_refs >= 0
    lookup = jnp.maximum(own_refs, 0)[:, None] == jnp.arange(owner_map.shape[0], dtype=jnp.int32)
    source = jnp.sum(jnp.where(lookup, owner_map, 0), axis=-1) // img_local
    position = jnp.arange(slot_count, dtype=jnp.int32)
    earlier = (source[:, None] == source[None, :]) & present[None, :] & (position[None, :] < position[:, None])
    slot_of = (source ^ me) * capacity + jnp.sum(earlier.astype(jnp.int32), axis=-1)
    named = media_pos[:, :, None] == jnp.arange(per_sequence, dtype=jnp.int32)
    slots = jnp.sum(jnp.where(named, slot_of.reshape(seq_local, 1, per_sequence), 0), axis=-1)
    slots = jnp.where(media_pos >= 0, slots, -1).reshape(tokens, 1)

    share = tokens // shards
    cols = model_width // groups
    cot = cotangent.reshape(tokens, feat_local)
    share_rows = jnp.zeros((share, model_width), BF16)
    for j in range(shards):
        piece = lax.dynamic_slice(cot, ((shard ^ j) * share, 0), (share, feat_local))
        piece = swap(piece, "fsdp", j) if j else piece
        share_rows = lax.dynamic_update_slice(share_rows, piece, (0, (shard ^ j) * feat_local))
    by_offset = []
    for d in range(groups):
        piece = lax.dynamic_slice(share_rows, (0, (me ^ d) * cols), (share, cols))
        by_offset.append(swap(piece, "dp", d) if d else piece)
    cot_blocks = gather_blocks(jnp.stack(by_offset), "fsdp")
    cot_rows = jnp.zeros((groups, shards, share, cols), BF16)
    for j, block in enumerate(cot_blocks):
        cot_rows = lax.dynamic_update_slice(cot_rows, block[:, None], (0, shard ^ j, 0, 0))
    cot_rows = cot_rows.reshape(groups * tokens, cols)

    lanes = head_local * head_size // chunks
    weight_rows = output_weight.reshape(head_local * head_size, model_width)
    out_grad = None
    contexts = []
    for chunk in range(chunks):
        context = attend(slots, queries, arrived[chunk], chunk, head_size)
        contexts.append(context)
        gathered = {0: context}
        for d in range(2, groups, 2):
            gathered[d] = swap(context, "dp", d)
        for d in range(0, groups, 2):
            gathered[d + 1] = swap(gathered[d], "dp", 1)
        out_grad = grad_part(gate_scale, cot_rows, [gathered[d] for d in range(groups)], chunk, chunks, out_grad)
    update = jnp.dot(jnp.concatenate(contexts, axis=1), weight_rows, preferred_element_type=F32)

    blocks = {
        j: lax.dynamic_slice(update, (0, (shard ^ j) * feat_local), (tokens, feat_local)) for j in range(shards)
    }
    step = 1
    while step < shards:
        kept = {}
        for j in blocks:
            if not j & step:
                kept[j] = blocks[j] + swap(blocks[j | step].astype(BF16), "fsdp", step).astype(F32)
        blocks = kept
        step *= 2
    layer_out = (text_states.reshape(tokens, feat_local).astype(F32) + gate_scale[0] * blocks[0]).astype(BF16)
    return (
        layer_out.reshape(seq_local, window, feat_local),
        out_grad.reshape(head_local, head_size, cols),
    )


def solution(mesh):
    in_specs = (
        P("dp", None, "fsdp"),
        P("dp", None, "fsdp"),
        P(),
        P(),
        P(),
        P(None, "fsdp", None),
        P(None, "fsdp", None),
        P("fsdp", None, None),
        P("dp", None, None),
        P(),
        P("dp", None),
        P(),
    )
    out_specs = (P("dp", None, "fsdp"), P("fsdp", None, "dp"))
    return jax.shard_map(body, mesh=mesh, in_specs=in_specs, out_specs=out_specs, check_vma=False)
```

```python
import functools

import jax
import jax.numpy as jnp
from jax import lax
from jax.experimental import pallas as pl
from jax.experimental.pallas import tpu as pltpu
from jax.sharding import PartitionSpec as P


EPSILON = 1e-05
F32 = jnp.float32
BF16 = jnp.bfloat16


def swap(value, axis, offset):
    size = lax.axis_size(axis)
    return lax.ppermute(value, axis, [(i, i ^ offset) for i in range(size)])


def layer_norm(row_values, norm_gain, norm_bias):
    as_float = row_values.astype(F32)
    row_mean = jnp.mean(as_float, axis=-1, keepdims=True)
    centered = as_float - row_mean
    variance = jnp.mean(centered * centered, axis=-1, keepdims=True)
    return (centered * lax.rsqrt(variance + EPSILON) * norm_gain + norm_bias).astype(BF16)


def gather_blocks(value, axis):
    size = lax.axis_size(axis)
    blocks = {0: value}
    step = size // 2
    while step:
        for offset in list(blocks):
            blocks[offset | step] = swap(blocks[offset], axis, step)
        step //= 2
    return [blocks[j] for j in range(size)]


def pairs_kernel(first, heads, groups, capacity, splits, me_ref, refs_ref, owner_ref, latent_hbm, weight_hbm, *rest):
    outs, (latent_buf, weight_buf, acc, pairs, picked, sems) = rest[:groups], rest[groups:]
    images_local, latent_rows = pairs.shape[1], pairs.shape[2]
    depth = latent_hbm.shape[1] // splits
    copies = []
    for k in range(splits):
        weight_copy = pltpu.make_async_copy(weight_hbm.at[pl.ds(k * depth, depth)], weight_buf.at[k], sems.at[2 * k])
        latent_copy = pltpu.make_async_copy(latent_hbm.at[:, pl.ds(k * depth, depth)], latent_buf.at[k], sems.at[2 * k + 1])
        weight_copy.start()
        latent_copy.start()
        copies.append((weight_copy, latent_copy))

    low = me_ref[0] * images_local
    per_sequence = refs_ref.shape[0]
    sequences = refs_ref.shape[1] // groups

    def per_target(offset, carry):
        for slot in range(capacity):
            picked[offset * (capacity + 1) + slot] = 0
        count = 0
        for sequence in range(sequences):
            for position in range(per_sequence):
                image = refs_ref[position, (me_ref[0] ^ offset) * sequences + sequence]
                within = owner_ref[jnp.maximum(image, 0)] - low
                hit = (image >= 0) & (within >= 0) & (within < images_local)
                slot = jnp.where(hit, jnp.minimum(count, capacity - 1), capacity)
                picked[offset * (capacity + 1) + slot] = within
                count = count + hit.astype(jnp.int32)
        return carry

    lax.fori_loop(0, groups, per_target, 0)
    sent = []
    for k in range(splits):
        copies[k][0].wait()
        copies[k][1].wait()
        weight = jnp.swapaxes(weight_buf[k], 0, 1)
        for head in range(heads):
            part = jnp.dot(latent_buf[k], weight[first + head], preferred_element_type=F32)
            if k:
                part = acc[head] + part
            if k < splits - 1:
                acc[head] = part
                continue
            pairs[head] = part.astype(BF16).reshape(pairs.shape[1:])
            for offset in reversed(range(groups)):
                for slot in range(capacity):
                    index = picked[offset * (capacity + 1) + slot]
                    target = outs[offset].at[head, pl.ds(slot * latent_rows, latent_rows)]
                    sent.append(pltpu.make_async_copy(pairs.at[head, index], target, sems.at[2 * splits + len(sent)]))
                    sent[-1].start()
    for copy in sent:
        copy.wait()


def outgoing_pairs(me, media_refs, owner_map, latents, weight, groups, capacity, first, heads):
    images_local, latent_rows, model_width = latents.shape
    width = weight.shape[2]
    rows = images_local * latent_rows
    splits = 4
    depth = model_width // splits
    smem = pl.BlockSpec(memory_space=pltpu.SMEM)
    hbm = pl.BlockSpec(memory_space=pl.ANY)
    return pl.pallas_call(
        functools.partial(pairs_kernel, first, heads, groups, capacity, splits),
        out_shape=[jax.ShapeDtypeStruct((heads, capacity * latent_rows, width), BF16)] * groups,
        in_specs=[smem, smem, smem, hbm, hbm],
        out_specs=[hbm] * groups,
        scratch_shapes=[
            pltpu.VMEM((splits, rows, depth), BF16),
            pltpu.VMEM((splits, depth, weight.shape[1], width), BF16),
            pltpu.VMEM((heads, rows, width), F32),
            pltpu.VMEM((heads, images_local, latent_rows, width), BF16),
            pltpu.SMEM((groups * (capacity + 1),), jnp.int32),
            pltpu.SemaphoreType.DMA((2 * splits + groups * capacity * heads,)),
        ],
        cost_estimate=pl.CostEstimate(
            flops=2 * rows * model_width * heads * width, bytes_accessed=latents.size * 2 + weight.size * 2, transcendentals=0
        ),
        name="pairs",
    )(me.reshape(1), media_refs.T, owner_map, latents.reshape(rows, model_width), weight)


def attend_kernel(latent_rows, base, count, slot_ref, query_ref, *rest):
    buffers, previous, out = rest[:count], rest[count:-1], rest[-1]
    heads, per_source, width = buffers[0].shape
    head_size = width // 2
    slot = slot_ref[...] - base
    columns = lax.broadcasted_iota(jnp.int32, (slot.shape[0], count * per_source), 1) // latent_rows
    allowed = columns == slot
    here = (slot >= 0) & (slot < count * (per_source // latent_rows))
    lanes = [slice(head * head_size, (head + 1) * head_size) for head in range(heads)]
    probs = []
    for head in range(heads):
        keys = jnp.concatenate([b[head, :, :head_size] for b in buffers], axis=0)
        scores = lax.dot_general(query_ref[:, lanes[head]], keys, (((1,), (1,)), ((), ())), preferred_element_type=F32)
        scores = jnp.where(allowed, scores, -1e30)
        weights = jnp.exp(scores - jnp.max(scores, axis=-1, keepdims=True))
        probs.append((weights / jnp.sum(weights, axis=-1, keepdims=True)).astype(BF16))
    contexts = []
    for head in range(heads):
        values = jnp.concatenate([b[head, :, head_size:] for b in buffers], axis=0)
        context = jnp.dot(probs[head], values, preferred_element_type=F32).astype(BF16)
        others = previous[0][:, lanes[head]] if previous else jnp.zeros(context.shape, BF16)
        contexts.append(jnp.where(here, context, others))
    out[...] = jnp.concatenate(contexts, axis=1)


def attend(slots, queries, arrived, base, latent_rows, previous):
    heads, _, width = arrived[0].shape
    tokens = queries.shape[0]
    lanes = heads * width // 2
    wide = pl.BlockSpec((tokens, lanes), lambda i: (0, 0))
    return pl.pallas_call(
        functools.partial(attend_kernel, latent_rows, base, len(arrived)),
        grid=(1,),
        out_shape=jax.ShapeDtypeStruct((tokens, lanes), BF16),
        in_specs=[pl.BlockSpec((tokens, 1), lambda i: (0, 0)), wide]
        + [pl.BlockSpec(arrived[0].shape, lambda i: (0, 0, 0))] * len(arrived)
        + [wide] * len(previous),
        out_specs=wide,
        name="attend",
    )(slots, queries, *arrived, *previous)


def grad_kernel(members, shards, place_ref, gate_ref, *rest):
    blocks, rest = rest[:shards], rest[shards:]
    contexts, previous, out, cot = rest[: len(members)], rest[len(members) : -2], rest[-2], rest[-1]
    for i, offset in enumerate(members):
        for j in range(shards):
            cot[i, place_ref[1] ^ j] = blocks[j][place_ref[0] ^ offset]
    rows = jnp.concatenate([c[...] for c in contexts], axis=0)
    columns = cot[...].reshape(rows.shape[0], out.shape[1])
    grad = gate_ref[0] * lax.dot_general(rows, columns, (((0,), (0,)), ((), ())), preferred_element_type=F32)
    out[...] = grad + previous[0][...] if previous else grad


def grad_part(place, gate, cot_blocks, contexts, members, previous):
    count = len(contexts)
    tokens, lanes = contexts[0].shape
    groups, share, cols = cot_blocks[0].shape
    total = pl.BlockSpec((lanes, cols), lambda i: (0, 0))
    smem = pl.BlockSpec(memory_space=pltpu.SMEM)
    return pl.pallas_call(
        functools.partial(grad_kernel, members, len(cot_blocks)),
        grid=(1,),
        out_shape=jax.ShapeDtypeStruct((lanes, cols), F32),
        in_specs=[smem, smem]
        + [pl.BlockSpec((groups, share, cols), lambda i: (0, 0, 0))] * len(cot_blocks)
        + [pl.BlockSpec((tokens, lanes), lambda i: (0, 0))] * count
        + [total] * len(previous),
        out_specs=total,
        scratch_shapes=[pltpu.VMEM((count, len(cot_blocks), share, cols), BF16)],
        input_output_aliases={2 + len(cot_blocks) + count: 0} if previous else {},
        name="grad",
    )(place, gate, *cot_blocks, *contexts, *previous)


def body(
    text_states,
    cotangent,
    norm_gain,
    norm_bias,
    branch_gate,
    query_weight,
    latent_weight,
    output_weight,
    latents,
    media_refs,
    media_pos,
    owner_map,
):
    seq_local, window, feat_local = text_states.shape
    model_width = query_weight.shape[0]
    head_local, head_size = query_weight.shape[1], query_weight.shape[2]
    img_local, latent_rows = latents.shape[0], latents.shape[1]
    groups, shards = lax.axis_size("dp"), lax.axis_size("fsdp")
    me, shard = lax.axis_index("dp"), lax.axis_index("fsdp")
    per_sequence = media_refs.shape[1]
    slot_count = media_refs.shape[0] * per_sequence // groups
    capacity = (slot_count + groups - 1) // groups
    tokens = seq_local * window
    gate_scale = jnp.tanh(branch_gate)

    outgoing = outgoing_pairs(me, media_refs, owner_map, latents, latent_weight, groups, capacity, 0, head_local)
    outgoing, text_in, cotangent = lax.optimization_barrier((outgoing, text_states, cotangent))
    half = groups // 2
    arrived = {0: outgoing[0]}
    for d in range(groups - 1, 0, -1):
        arrived[d] = swap(outgoing[d], "dp", d)

    text_blocks = gather_blocks(text_in.reshape(tokens, feat_local), "fsdp")
    text_rows = jnp.zeros((tokens, model_width), BF16)
    for j, block in enumerate(text_blocks):
        text_rows = lax.dynamic_update_slice(text_rows, block, (0, (shard ^ j) * feat_local))
    normed = layer_norm(text_rows, norm_gain, norm_bias)
    queries = jnp.dot(normed, query_weight.reshape(model_width, head_local * head_size), preferred_element_type=F32)
    queries = (queries * head_size ** (-0.5)).astype(BF16)

    own_refs = lax.dynamic_slice_in_dim(media_refs, me * seq_local, seq_local, 0).reshape(slot_count)
    present = own_refs >= 0
    lookup = jnp.maximum(own_refs, 0)[:, None] == jnp.arange(owner_map.shape[0], dtype=jnp.int32)
    source = jnp.sum(jnp.where(lookup, owner_map, 0), axis=-1) // img_local
    position = jnp.arange(slot_count, dtype=jnp.int32)
    earlier = (source[:, None] == source[None, :]) & present[None, :] & (position[None, :] < position[:, None])
    slot_of = (source ^ me) * capacity + jnp.sum(earlier.astype(jnp.int32), axis=-1)
    named = media_pos[:, :, None] == jnp.arange(per_sequence, dtype=jnp.int32)
    slots = jnp.sum(jnp.where(named, slot_of.reshape(seq_local, 1, per_sequence), 0), axis=-1)
    slots = jnp.where(media_pos >= 0, slots, -1).reshape(tokens, 1)

    share = tokens // shards
    cols = model_width // groups
    cot = cotangent.reshape(tokens, feat_local)
    share_rows = jnp.zeros((shards, share, feat_local), BF16)
    for j in range(shards):
        piece = lax.dynamic_slice(cot, ((shard ^ j) * share, 0), (share, feat_local))
        piece = swap(piece, "fsdp", j) if j else piece
        share_rows = lax.dynamic_update_slice(share_rows, piece[None], (shard ^ j, 0, 0))
    share_rows = share_rows.reshape(shards, share, feat_local // cols, cols).transpose(0, 2, 1, 3)
    share_rows = lax.all_to_all(share_rows.reshape(groups, share, cols), "dp", 0, 0, tiled=True)
    cot_blocks = gather_blocks(share_rows, "fsdp")

    context = attend(slots, queries, [arrived[d] for d in range(half)], 0, latent_rows, [])
    context = attend(slots, queries, [arrived[d] for d in range(half, groups)], half * capacity, latent_rows, [context])
    gathered = {0: context}
    for d in range(groups - 2, 0, -2):
        gathered[d] = swap(context, "dp", d)
    gathered[1] = swap(context, "dp", 1)
    for d in range(2, groups, 2):
        gathered[d + 1] = swap(gathered[d], "dp", 1)

    place = jnp.stack([me, shard])
    last = max(groups - 2, groups // 2)
    out_grad = []
    for members in (range(last), range(last, groups)):
        group_contexts = [gathered[d] for d in members]
        out_grad = [grad_part(place, gate_scale, cot_blocks, group_contexts, tuple(members), out_grad)]
    out_grad = out_grad[0]
    update = jnp.dot(context, output_weight.reshape(head_local * head_size, model_width), preferred_element_type=F32)

    blocks = {
        j: lax.dynamic_slice(update, (0, (shard ^ j) * feat_local), (tokens, feat_local)) for j in range(shards)
    }
    step = 1
    while step < shards:
        kept = {}
        for j in blocks:
            if not j & step:
                received = swap(blocks[j | step].astype(BF16), "fsdp", step)
                kept[j] = blocks[j] + received.astype(F32)
        blocks = kept
        step *= 2
    layer_out = (text_states.reshape(tokens, feat_local).astype(F32) + gate_scale[0] * blocks[0]).astype(BF16)
    return (
        layer_out.reshape(seq_local, window, feat_local),
        out_grad.reshape(head_local, head_size, cols),
    )


def solution(mesh):
    in_specs = (
        P("dp", None, "fsdp"),
        P("dp", None, "fsdp"),
        P(),
        P(),
        P(),
        P(None, "fsdp", None),
        P(None, "fsdp", None),
        P("fsdp", None, None),
        P("dp", None, None),
        P(),
        P("dp", None),
        P(),
    )
    out_specs = (P("dp", None, "fsdp"), P("fsdp", None, "dp"))

    return jax.shard_map(body, mesh=mesh, in_specs=in_specs, out_specs=out_specs, check_vma=False)
```

```python
import functools

import jax
import jax.numpy as jnp
from jax import lax
from jax.experimental import pallas as pl
from jax.experimental.pallas import tpu as pltpu
from jax.sharding import PartitionSpec as P


EPSILON = 1e-05
F32 = jnp.float32
BF16 = jnp.bfloat16


VMEM = pl.BlockSpec(memory_space=pltpu.VMEM)
SMEM = pl.BlockSpec(memory_space=pltpu.SMEM)


def limit(mebibytes):
    return pltpu.CompilerParams(vmem_limit_bytes=mebibytes << 20)


def swap(value, axis, offset):
    size = lax.axis_size(axis)
    return lax.ppermute(value, axis, [(i, i ^ offset) for i in range(size)])


def norm_kernel(shards, place_ref, gain_ref, bias_ref, *rest):
    blocks, out = rest[:shards], rest[shards]
    feats = blocks[0].shape[1]
    width = shards * feats
    mean = sum(jnp.sum(block[...].astype(F32), axis=-1, keepdims=True) for block in blocks) / width
    squares = 0.0
    for block in blocks:
        centered = block[...].astype(F32) - mean
        squares = squares + jnp.sum(centered * centered, axis=-1, keepdims=True)
    scaling = lax.rsqrt(squares / width + EPSILON)
    for j, block in enumerate(blocks):
        columns = pl.ds(pl.multiple_of((place_ref[1] ^ j) * feats, 128), feats)
        centered = block[...].astype(F32) - mean
        out[:, columns] = (centered * scaling * gain_ref[:, columns] + bias_ref[:, columns]).astype(BF16)


def norm_rows(place, norm_gain, norm_bias, text_blocks):
    tokens, _ = text_blocks[0].shape
    width = norm_gain.shape[0]
    return pl.pallas_call(
        functools.partial(norm_kernel, len(text_blocks)),
        out_shape=jax.ShapeDtypeStruct((tokens, width), BF16),
        in_specs=[SMEM] + [VMEM] * (2 + len(text_blocks)),
        out_specs=VMEM,
        compiler_params=limit(12),
        name="norm",
    )(place, norm_gain.reshape(1, width), norm_bias.reshape(1, width), *text_blocks)


def gather_blocks(value, axis):
    size = lax.axis_size(axis)
    blocks = {0: value}
    step = size // 2
    while step:
        for offset in list(blocks):
            blocks[offset | step] = swap(blocks[offset], axis, step)
        step //= 2
    return [blocks[j] for j in range(size)]


def pairs_kernel(chunks, heads, groups, capacity, splits, me_ref, refs_ref, owner_ref, latent_hbm, weight_hbm, *rest):
    half = groups // 2
    outs, (latent_buf, weight_buf, acc, pairs, picked, sems) = rest[: half * chunks], rest[half * chunks :]
    images_local, latent_rows = pairs.shape[1], pairs.shape[2]
    depth = latent_hbm.shape[1] // splits
    copies = []
    for k in range(splits):
        weight_copy = pltpu.make_async_copy(weight_hbm.at[pl.ds(k * depth, depth)], weight_buf.at[k], sems.at[2 * k])
        latent_copy = pltpu.make_async_copy(latent_hbm.at[:, pl.ds(k * depth, depth)], latent_buf.at[k], sems.at[2 * k + 1])
        weight_copy.start()
        latent_copy.start()
        copies.append((weight_copy, latent_copy))

    low = me_ref[0] * images_local
    per_sequence = refs_ref.shape[0]
    sequences = refs_ref.shape[1] // groups

    def per_target(offset, carry):
        for slot in range(capacity):
            picked[offset * (capacity + 1) + slot] = 0
        count = 0
        for sequence in range(sequences):
            for position in range(per_sequence):
                image = refs_ref[position, (me_ref[0] ^ offset) * sequences + sequence]
                within = owner_ref[jnp.maximum(image, 0)] - low
                hit = (image >= 0) & (within >= 0) & (within < images_local)
                slot = jnp.where(hit, jnp.minimum(count, capacity - 1), capacity)
                picked[offset * (capacity + 1) + slot] = within
                count = count + hit.astype(jnp.int32)
        return carry

    lax.fori_loop(0, groups, per_target, 0)
    sent = []
    for k in range(splits):
        copies[k][0].wait()
        copies[k][1].wait()
        weight = jnp.swapaxes(weight_buf[k], 0, 1)
        for head in range(heads):
            part = jnp.dot(latent_buf[k], weight[head], preferred_element_type=F32)
            if k:
                part = acc[head] + part
            if k < splits - 1:
                acc[head] = part
                continue
            pairs[head] = part.astype(BF16).reshape(pairs.shape[1:])
            chunk, row = head // (heads // chunks), head % (heads // chunks)
            for offset in reversed(range(groups)):
                out = outs[chunk * half + offset % half]
                for slot in range(capacity):
                    index = picked[offset * (capacity + 1) + slot]
                    place = pl.ds((offset // half * capacity + slot) * latent_rows, latent_rows)
                    sent.append(
                        pltpu.make_async_copy(pairs.at[head, index], out.at[row, place], sems.at[2 * splits + len(sent)])
                    )
                    sent[-1].start()
    for copy in sent:
        copy.wait()


def outgoing_pairs(me, media_refs, owner_map, latents, weight, groups, capacity, chunks):
    images_local, latent_rows, model_width = latents.shape
    heads, width = weight.shape[1:]
    rows = images_local * latent_rows
    half = groups // 2
    splits = 4
    depth = model_width // splits
    hbm = pl.BlockSpec(memory_space=pl.ANY)
    shape = (heads // chunks, 2 * capacity * latent_rows, width)
    outs = pl.pallas_call(
        functools.partial(pairs_kernel, chunks, heads, groups, capacity, splits),
        out_shape=[jax.ShapeDtypeStruct(shape, BF16)] * (half * chunks),
        in_specs=[SMEM, SMEM, SMEM, hbm, hbm],
        out_specs=[hbm] * (half * chunks),
        scratch_shapes=[
            pltpu.VMEM((splits, rows, depth), BF16),
            pltpu.VMEM((splits, depth, heads, width), BF16),
            pltpu.VMEM((heads, rows, width), F32),
            pltpu.VMEM((heads, images_local, latent_rows, width), BF16),
            pltpu.SMEM((groups * (capacity + 1),), jnp.int32),
            pltpu.SemaphoreType.DMA((2 * splits + groups * capacity * heads,)),
        ],
        cost_estimate=pl.CostEstimate(
            flops=2 * rows * model_width * heads * width, bytes_accessed=latents.size * 2 + weight.size * 2, transcendentals=0
        ),
        name="pairs",
    )(me.reshape(1), media_refs.T, owner_map, latents.reshape(rows, model_width), weight)
    return [outs[chunk * half : (chunk + 1) * half] for chunk in range(chunks)]


def attend_kernel(latent_rows, chunk, count, own_slot_ref, far_slot_ref, own_query_ref, far_query_ref, *rest):
    buffers, out = rest[:count], rest[count]
    heads, both, width = buffers[0].shape
    head_size = width // 2
    per_source = both // 2
    slots = count * per_source // latent_rows
    sides = ((own_slot_ref[...], own_query_ref, 0), (far_slot_ref[...] - slots, far_query_ref, per_source))
    columns = lax.broadcasted_iota(jnp.int32, (own_slot_ref.shape[0], count * per_source), 1) // latent_rows
    lanes = [slice((chunk * heads + head) * head_size, (chunk * heads + head + 1) * head_size) for head in range(heads)]
    probs = []
    for slot, query_ref, first in sides:
        allowed = columns == slot
        for head in range(heads):
            keys = jnp.concatenate([b[head, first : first + per_source, :head_size] for b in buffers], axis=0)
            scores = lax.dot_general(
                query_ref[:, lanes[head]], keys, (((1,), (1,)), ((), ())), preferred_element_type=F32
            )
            scores = jnp.where(allowed, scores, -1e30)
            weights = jnp.exp(scores - jnp.max(scores, axis=-1, keepdims=True))
            probs.append((weights / jnp.sum(weights, axis=-1, keepdims=True)).astype(BF16))
    contexts = []
    for side, (slot, query_ref, first) in enumerate(sides):
        here = (slot >= 0) & (slot < slots)
        for head in range(heads):
            values = jnp.concatenate([b[head, first : first + per_source, head_size:] for b in buffers], axis=0)
            context = jnp.dot(probs[side * heads + head], values, preferred_element_type=F32)
            contexts.append(jnp.where(here, context, 0.0).astype(BF16))
    for side in range(2):
        out[side] = jnp.concatenate(contexts[side * heads : (side + 1) * heads], axis=1)


def attend(own_slots, far_slots, own_queries, far_queries, arrived, chunk, latent_rows):
    heads, _, width = arrived[0].shape
    return pl.pallas_call(
        functools.partial(attend_kernel, latent_rows, chunk, len(arrived)),
        out_shape=jax.ShapeDtypeStruct((2, own_queries.shape[0], heads * width // 2), BF16),
        in_specs=[VMEM] * (4 + len(arrived)),
        out_specs=VMEM,
        compiler_params=limit(12),
        name="attend",
    )(own_slots, far_slots, own_queries, far_queries, *arrived)


def join_kernel(mine_ref, other_ref, out):
    for side in range(2):
        out[side] = mine_ref[side] + other_ref[1 - side]


def join(mine, other):
    return pl.pallas_call(
        join_kernel,
        out_shape=jax.ShapeDtypeStruct(mine.shape, mine.dtype),
        in_specs=[VMEM] * 2,
        out_specs=VMEM,
        compiler_params=limit(4),
        name="join",
    )(mine, other)


def update_kernel(shards, chunks, place_ref, weight_hbm, *rest):
    contexts, outs, (weight_buf, sems) = rest[:chunks], rest[chunks : chunks + shards], rest[chunks + shards :]
    feats = outs[0].shape[1]
    copies = []
    for j in range(shards):
        columns = pl.ds(pl.multiple_of((place_ref[1] ^ j) * feats, 128), feats)
        copies.append(pltpu.make_async_copy(weight_hbm.at[:, columns], weight_buf.at[j], sems.at[j]))
    for j in reversed(range(shards)):
        copies[j].start()
    rows = jnp.concatenate([c[0] for c in contexts], axis=1)
    for j in reversed(range(shards)):
        copies[j].wait()
        outs[j][...] = jnp.dot(rows, weight_buf[j], preferred_element_type=F32).astype(BF16)


def update_terms(place, contexts, weight, shards):
    tokens, feats = contexts[0].shape[1], weight.shape[1] // shards
    return pl.pallas_call(
        functools.partial(update_kernel, shards, len(contexts)),
        in_specs=[SMEM, pl.BlockSpec(memory_space=pltpu.HBM)] + [VMEM] * len(contexts),
        out_specs=[VMEM] * shards,
        out_shape=[jax.ShapeDtypeStruct((tokens, feats), BF16)] * shards,
        scratch_shapes=[pltpu.VMEM((shards, weight.shape[0], feats), BF16), pltpu.SemaphoreType.DMA((shards,))],
        compiler_params=limit(20),
        name="update",
    )(place, weight, *contexts)


def grad_kernel(count, place_ref, gate_ref, cot_ref, *rest):
    contexts, previous, out, rows = rest[:count], rest[count:-2], rest[-2], rest[-1]
    for offset in range(count):
        for side in range(2):
            rows[place_ref[0] ^ (offset + side * count)] = contexts[offset][side]
    tokens, lanes = cot_ref.shape[0], rows.shape[2]
    grad = lax.dot_general(
        rows[...].reshape(tokens, lanes), cot_ref[...], (((0,), (0,)), ((), ())), preferred_element_type=F32
    )
    if previous:
        out[: out.shape[0] - lanes] = previous[0][...]
    out[out.shape[0] - lanes :] = gate_ref[0] * grad


def grad_part(place, gate, cot_rows, contexts, previous):
    count = len(contexts)
    _, tokens, lanes = contexts[0].shape
    rows = lanes + (previous[0].shape[0] if previous else 0)
    return pl.pallas_call(
        functools.partial(grad_kernel, count),
        out_shape=jax.ShapeDtypeStruct((rows, cot_rows.shape[1]), F32),
        in_specs=[SMEM] * 2 + [VMEM] * (1 + count + len(previous)),
        out_specs=VMEM,
        scratch_shapes=[pltpu.VMEM((2 * count, tokens, lanes), BF16)],
        compiler_params=limit(16),
        name="grad",
    )(place, gate, cot_rows, *contexts, *previous)


def body(
    text_states,
    cotangent,
    norm_gain,
    norm_bias,
    branch_gate,
    query_weight,
    latent_weight,
    output_weight,
    latents,
    media_refs,
    media_pos,
    owner_map,
):
    seq_local, window, feat_local = text_states.shape
    model_width = query_weight.shape[0]
    head_local, head_size = query_weight.shape[1], query_weight.shape[2]
    img_local, latent_rows = latents.shape[0], latents.shape[1]
    groups, shards = lax.axis_size("dp"), lax.axis_size("fsdp")
    me, shard = lax.axis_index("dp"), lax.axis_index("fsdp")
    per_sequence = media_refs.shape[1]
    slot_count = media_refs.shape[0] * per_sequence // groups
    capacity = (slot_count + groups - 1) // groups
    tokens = seq_local * window
    gate_scale = jnp.tanh(branch_gate)

    half = groups // 2
    chunks = 2 if head_local % 2 == 0 else 1
    place = jnp.stack([me, shard])

    far_pos = swap(media_pos, "dp", half)
    text_blocks = gather_blocks(text_states.reshape(tokens, feat_local), "fsdp")
    outgoing = outgoing_pairs(me, media_refs, owner_map, latents, latent_weight, groups, capacity, chunks)
    arrived = []
    for chunk in range(chunks):
        received = {o: swap(outgoing[chunk][o], "dp", o) for o in range(half - 1, 0, -1)}
        arrived.append([outgoing[chunk][0]] + [received[o] for o in range(1, half)])

    normed = norm_rows(place, norm_gain, norm_bias, text_blocks)
    queries = jnp.dot(normed, query_weight.reshape(model_width, head_local * head_size), preferred_element_type=F32)
    queries = (queries * head_size ** (-0.5)).astype(BF16)
    far_queries = swap(queries, "dp", half)

    tables = (queries, media_pos, far_pos, media_refs, owner_map)
    queries, media_pos, far_pos, media_refs, owner_map = lax.optimization_barrier(tables)

    def slots_of(group, positions):
        refs = lax.dynamic_slice_in_dim(media_refs, group * seq_local, seq_local, 0).reshape(slot_count)
        present = refs >= 0
        lookup = jnp.maximum(refs, 0)[:, None] == jnp.arange(owner_map.shape[0], dtype=jnp.int32)
        source = jnp.sum(jnp.where(lookup, owner_map, 0), axis=-1) // img_local
        position = jnp.arange(slot_count, dtype=jnp.int32)
        earlier = (source[:, None] == source[None, :]) & present[None, :] & (position[None, :] < position[:, None])
        slot_of = (source ^ group) * capacity + jnp.sum(earlier.astype(jnp.int32), axis=-1)
        named = positions[:, :, None] == jnp.arange(per_sequence, dtype=jnp.int32)
        slots = jnp.sum(jnp.where(named, slot_of.reshape(seq_local, 1, per_sequence), 0), axis=-1)
        return jnp.where(positions >= 0, slots, -1).reshape(tokens, 1)

    own_slots = slots_of(me, media_pos)
    far_slots = slots_of(me ^ half, far_pos)

    share = tokens // shards
    cols = model_width // groups
    cot = cotangent.reshape(tokens, feat_local)
    pieces = []
    for j in range(shards):
        piece = lax.dynamic_slice(cot, ((shard ^ j) * share, 0), (share, feat_local))
        pieces.append(swap(piece, "fsdp", j) if j else piece)
    pieces, queries = lax.optimization_barrier((pieces, queries))
    share_rows = jnp.zeros((shards, share, feat_local), BF16)
    for j in range(shards):
        share_rows = lax.dynamic_update_slice(share_rows, pieces[j][None], (shard ^ j, 0, 0))
    share_rows = share_rows.reshape(shards, share, feat_local // cols, cols).transpose(0, 2, 1, 3)
    share_rows = lax.all_to_all(share_rows.reshape(groups, share, cols), "dp", 0, 0, tiled=True)
    cot_blocks = gather_blocks(share_rows, "fsdp")
    cot_rows = jnp.zeros((groups, shards, share, cols), BF16)
    for j, block in enumerate(cot_blocks):
        cot_rows = lax.dynamic_update_slice(cot_rows, block[:, None], (0, shard ^ j, 0, 0))
    cot_rows = cot_rows.reshape(groups * tokens, cols)

    contexts, out_grad = [], []
    for chunk in range(chunks):
        partial = attend(own_slots, far_slots, queries, far_queries, arrived[chunk], chunk, latent_rows)
        other = swap(partial, "dp", half)
        context = join(partial, other)
        contexts.append(context)
        gathered = {0: context}
        for o in range(half - 2, 0, -2):
            gathered[o] = swap(context, "dp", o)
        gathered[1] = swap(context, "dp", 1)
        for o in range(half - 2, 0, -2):
            gathered[o + 1] = swap(gathered[o], "dp", 1)
        group_contexts = [gathered[o] for o in range(half)]
        out_grad = [grad_part(place, gate_scale, cot_rows, group_contexts, out_grad)]
    out_grad = out_grad[0]

    weight_rows = output_weight.reshape(head_local * head_size, model_width)
    blocks = dict(enumerate(update_terms(place, contexts, weight_rows, shards)))
    step = 1
    while step < shards:
        kept = {}
        for j in blocks:
            if not j & step:
                received = swap(blocks[j | step].astype(BF16), "fsdp", step)
                kept[j] = blocks[j].astype(F32) + received.astype(F32)
        blocks = kept
        step *= 2
    layer_out = (text_states.reshape(tokens, feat_local).astype(F32) + gate_scale[0] * blocks[0]).astype(BF16)
    return (
        layer_out.reshape(seq_local, window, feat_local),
        out_grad.reshape(head_local, head_size, cols),
    )


def solution(mesh):
    in_specs = (
        P("dp", None, "fsdp"),
        P("dp", None, "fsdp"),
        P(),
        P(),
        P(),
        P(None, "fsdp", None),
        P(None, "fsdp", None),
        P("fsdp", None, None),
        P("dp", None, None),
        P(),
        P("dp", None),
        P(),
    )
    out_specs = (P("dp", None, "fsdp"), P("fsdp", None, "dp"))

    return jax.shard_map(body, mesh=mesh, in_specs=in_specs, out_specs=out_specs, check_vma=False)
```

```python
import functools

import jax
import jax.numpy as jnp
from jax import lax
from jax.experimental import pallas as pl
from jax.experimental.pallas import tpu as pltpu
from jax.sharding import PartitionSpec as P


EPSILON = 1e-05
F32 = jnp.float32
BF16 = jnp.bfloat16


VMEM = pl.BlockSpec(memory_space=pltpu.VMEM)
SMEM = pl.BlockSpec(memory_space=pltpu.SMEM)


def limit(mebibytes):
    return pltpu.CompilerParams(vmem_limit_bytes=mebibytes << 20)


def swap(value, axis, offset):
    size = lax.axis_size(axis)
    return lax.ppermute(value, axis, [(i, i ^ offset) for i in range(size)])


def norm_kernel(shards, place_ref, gain_ref, bias_ref, *rest):
    blocks, out = rest[:shards], rest[shards]
    feats = blocks[0].shape[1]
    width = shards * feats
    mean = sum(jnp.sum(block[...].astype(F32), axis=-1, keepdims=True) for block in blocks) / width
    squares = 0.0
    for block in blocks:
        centered = block[...].astype(F32) - mean
        squares = squares + jnp.sum(centered * centered, axis=-1, keepdims=True)
    scaling = lax.rsqrt(squares / width + EPSILON)
    for j, block in enumerate(blocks):
        columns = pl.ds(pl.multiple_of((place_ref[1] ^ j) * feats, 128), feats)
        centered = block[...].astype(F32) - mean
        out[:, columns] = (centered * scaling * gain_ref[:, columns] + bias_ref[:, columns]).astype(BF16)


def norm_rows(place, norm_gain, norm_bias, text_blocks):
    tokens, _ = text_blocks[0].shape
    width = norm_gain.shape[0]
    return pl.pallas_call(
        functools.partial(norm_kernel, len(text_blocks)),
        out_shape=jax.ShapeDtypeStruct((tokens, width), BF16),
        in_specs=[SMEM] + [VMEM] * (2 + len(text_blocks)),
        out_specs=VMEM,
        compiler_params=limit(12),
        name="norm",
    )(place, norm_gain.reshape(1, width), norm_bias.reshape(1, width), *text_blocks)


def gather_blocks(value, axis):
    size = lax.axis_size(axis)
    blocks = {0: value}
    step = size // 2
    while step:
        for offset in list(blocks):
            blocks[offset | step] = swap(blocks[offset], axis, step)
        step //= 2
    return [blocks[j] for j in range(size)]


def pairs_kernel(chunks, heads, groups, capacity, splits, refs_hbm, owner_hbm, latent_hbm, weight_hbm, *rest):
    half = groups // 2
    outs = rest[: half * chunks]
    latent_buf, weight_buf, acc, pairs, refs_ref, owner_ref, picked, sems, table_sems = rest[half * chunks :]
    me = lax.axis_index("dp")
    images_local, latent_rows = pairs.shape[1], pairs.shape[2]
    depth = latent_hbm.shape[1] // splits
    copies = []
    for k in range(splits):
        weight_copy = pltpu.make_async_copy(weight_hbm.at[pl.ds(k * depth, depth)], weight_buf.at[k], sems.at[2 * k])
        latent_copy = pltpu.make_async_copy(latent_hbm.at[:, pl.ds(k * depth, depth)], latent_buf.at[k], sems.at[2 * k + 1])
        weight_copy.start()
        latent_copy.start()
        copies.append((weight_copy, latent_copy))

    tables = (
        pltpu.make_async_copy(refs_hbm, refs_ref, table_sems.at[0]),
        pltpu.make_async_copy(owner_hbm, owner_ref, table_sems.at[1]),
    )
    for table in tables:
        table.start()
    for table in tables:
        table.wait()

    low = me * images_local
    per_sequence = refs_ref.shape[0]
    sequences = refs_ref.shape[1] // groups

    def per_target(offset, carry):
        for slot in range(capacity):
            picked[offset * (capacity + 1) + slot] = 0
        count = 0
        for sequence in range(sequences):
            for position in range(per_sequence):
                image = refs_ref[position, (me ^ offset) * sequences + sequence]
                within = owner_ref[jnp.maximum(image, 0)] - low
                hit = (image >= 0) & (within >= 0) & (within < images_local)
                slot = jnp.where(hit, jnp.minimum(count, capacity - 1), capacity)
                picked[offset * (capacity + 1) + slot] = within
                count = count + hit.astype(jnp.int32)
        return carry

    lax.fori_loop(0, groups, per_target, 0)
    sent = []
    for k in range(splits):
        copies[k][0].wait()
        copies[k][1].wait()
        weight = jnp.swapaxes(weight_buf[k], 0, 1)
        for head in range(heads):
            part = jnp.dot(latent_buf[k], weight[head], preferred_element_type=F32)
            if k:
                part = acc[head] + part
            if k < splits - 1:
                acc[head] = part
                continue
            pairs[head] = part.astype(BF16).reshape(pairs.shape[1:])
            chunk, row = head // (heads // chunks), head % (heads // chunks)
            for offset in reversed(range(groups)):
                out = outs[chunk * half + offset % half]
                for slot in range(capacity):
                    index = picked[offset * (capacity + 1) + slot]
                    place = pl.ds((offset // half * capacity + slot) * latent_rows, latent_rows)
                    sent.append(
                        pltpu.make_async_copy(pairs.at[head, index], out.at[row, place], sems.at[2 * splits + len(sent)])
                    )
                    sent[-1].start()
    for copy in sent:
        copy.wait()


def outgoing_pairs(media_refs, owner_map, latents, weight, groups, capacity, chunks):
    images_local, latent_rows, model_width = latents.shape
    heads, width = weight.shape[1:]
    rows = images_local * latent_rows
    half = groups // 2
    splits = 4
    depth = model_width // splits
    hbm = pl.BlockSpec(memory_space=pl.ANY)
    shape = (heads // chunks, 2 * capacity * latent_rows, width)
    outs = pl.pallas_call(
        functools.partial(pairs_kernel, chunks, heads, groups, capacity, splits),
        out_shape=[jax.ShapeDtypeStruct(shape, BF16)] * (half * chunks),
        in_specs=[hbm] * 4,
        out_specs=[hbm] * (half * chunks),
        scratch_shapes=[
            pltpu.VMEM((splits, rows, depth), BF16),
            pltpu.VMEM((splits, depth, heads, width), BF16),
            pltpu.VMEM((heads, rows, width), F32),
            pltpu.VMEM((heads, images_local, latent_rows, width), BF16),
            pltpu.SMEM(media_refs.shape[::-1], jnp.int32),
            pltpu.SMEM(owner_map.shape, jnp.int32),
            pltpu.SMEM((groups * (capacity + 1),), jnp.int32),
            pltpu.SemaphoreType.DMA((2 * splits + groups * capacity * heads,)),
            pltpu.SemaphoreType.DMA((2,)),
        ],
        cost_estimate=pl.CostEstimate(
            flops=2 * rows * model_width * heads * width, bytes_accessed=latents.size * 2 + weight.size * 2, transcendentals=0
        ),
        name="pairs",
    )(media_refs.T, owner_map, latents.reshape(rows, model_width), weight)
    return [outs[chunk * half : (chunk + 1) * half] for chunk in range(chunks)]


def attend_kernel(latent_rows, chunk, count, own_slot_ref, far_slot_ref, own_query_ref, far_query_ref, *rest):
    buffers, out = rest[:count], rest[count]
    heads, both, width = buffers[0].shape
    head_size = width // 2
    per_source = both // 2
    slots = count * per_source // latent_rows
    sides = ((own_slot_ref[...], own_query_ref, 0), (far_slot_ref[...] - slots, far_query_ref, per_source))
    columns = lax.broadcasted_iota(jnp.int32, (own_slot_ref.shape[0], count * per_source), 1) // latent_rows
    lanes = [slice((chunk * heads + head) * head_size, (chunk * heads + head + 1) * head_size) for head in range(heads)]
    probs = []
    for slot, query_ref, first in sides:
        allowed = columns == slot
        for head in range(heads):
            keys = jnp.concatenate([b[head, first : first + per_source, :head_size] for b in buffers], axis=0)
            scores = lax.dot_general(
                query_ref[:, lanes[head]], keys, (((1,), (1,)), ((), ())), preferred_element_type=F32
            )
            scores = jnp.where(allowed, scores, -1e30)
            weights = jnp.exp(scores - jnp.max(scores, axis=-1, keepdims=True))
            probs.append((weights / jnp.sum(weights, axis=-1, keepdims=True)).astype(BF16))
    contexts = []
    for side, (slot, query_ref, first) in enumerate(sides):
        here = (slot >= 0) & (slot < slots)
        for head in range(heads):
            values = jnp.concatenate([b[head, first : first + per_source, head_size:] for b in buffers], axis=0)
            context = jnp.dot(probs[side * heads + head], values, preferred_element_type=F32)
            contexts.append(jnp.where(here, context, 0.0).astype(BF16))
    for side in range(2):
        out[side] = jnp.concatenate(contexts[side * heads : (side + 1) * heads], axis=1)


def attend(own_slots, far_slots, own_queries, far_queries, arrived, chunk, latent_rows):
    heads, _, width = arrived[0].shape
    return pl.pallas_call(
        functools.partial(attend_kernel, latent_rows, chunk, len(arrived)),
        out_shape=jax.ShapeDtypeStruct((2, own_queries.shape[0], heads * width // 2), BF16),
        in_specs=[VMEM] * (4 + len(arrived)),
        out_specs=VMEM,
        compiler_params=limit(12),
        name="attend",
    )(own_slots, far_slots, own_queries, far_queries, *arrived)


def join_kernel(mine_ref, other_ref, out):
    for side in range(2):
        out[side] = mine_ref[side] + other_ref[1 - side]


def join(mine, other):
    return pl.pallas_call(
        join_kernel,
        out_shape=jax.ShapeDtypeStruct(mine.shape, mine.dtype),
        in_specs=[VMEM] * 2,
        out_specs=VMEM,
        compiler_params=limit(4),
        name="join",
    )(mine, other)


def update_kernel(shards, chunks, place_ref, weight_hbm, *rest):
    contexts, outs, (weight_buf, sems) = rest[:chunks], rest[chunks : chunks + shards], rest[chunks + shards :]
    feats = outs[0].shape[1]
    copies = []
    for j in range(shards):
        columns = pl.ds(pl.multiple_of((place_ref[1] ^ j) * feats, 128), feats)
        copies.append(pltpu.make_async_copy(weight_hbm.at[:, columns], weight_buf.at[j], sems.at[j]))
    for j in reversed(range(shards)):
        copies[j].start()
    rows = jnp.concatenate([c[0] for c in contexts], axis=1)
    for j in reversed(range(shards)):
        copies[j].wait()
        outs[j][...] = jnp.dot(rows, weight_buf[j], preferred_element_type=F32).astype(BF16)


def update_terms(place, contexts, weight, shards):
    tokens, feats = contexts[0].shape[1], weight.shape[1] // shards
    return pl.pallas_call(
        functools.partial(update_kernel, shards, len(contexts)),
        in_specs=[SMEM, pl.BlockSpec(memory_space=pltpu.HBM)] + [VMEM] * len(contexts),
        out_specs=[VMEM] * shards,
        out_shape=[jax.ShapeDtypeStruct((tokens, feats), BF16)] * shards,
        scratch_shapes=[pltpu.VMEM((shards, weight.shape[0], feats), BF16), pltpu.SemaphoreType.DMA((shards,))],
        name="update",
    )(place, weight, *contexts)


def grad_kernel(count, place_ref, gate_ref, cot_ref, *rest):
    contexts, previous, out, rows = rest[:count], rest[count:-2], rest[-2], rest[-1]
    for offset in range(count):
        for side in range(2):
            rows[place_ref[0] ^ (offset + side * count)] = contexts[offset][side]
    tokens, lanes = cot_ref.shape[0], rows.shape[2]
    grad = lax.dot_general(
        rows[...].reshape(tokens, lanes), cot_ref[...], (((0,), (0,)), ((), ())), preferred_element_type=F32
    )
    if previous:
        out[: out.shape[0] - lanes] = previous[0][...]
    out[out.shape[0] - lanes :] = gate_ref[0] * grad


def grad_part(place, gate, cot_rows, contexts, previous):
    count = len(contexts)
    _, tokens, lanes = contexts[0].shape
    rows = lanes + (previous[0].shape[0] if previous else 0)
    return pl.pallas_call(
        functools.partial(grad_kernel, count),
        out_shape=jax.ShapeDtypeStruct((rows, cot_rows.shape[1]), F32),
        in_specs=[SMEM] * 2 + [VMEM] * (1 + count + len(previous)),
        out_specs=VMEM,
        scratch_shapes=[pltpu.VMEM((2 * count, tokens, lanes), BF16)],
        compiler_params=limit(16),
        name="grad",
    )(place, gate, cot_rows, *contexts, *previous)


def body(
    text_states,
    cotangent,
    norm_gain,
    norm_bias,
    branch_gate,
    query_weight,
    latent_weight,
    output_weight,
    latents,
    media_refs,
    media_pos,
    owner_map,
):
    seq_local, window, feat_local = text_states.shape
    model_width = query_weight.shape[0]
    head_local, head_size = query_weight.shape[1], query_weight.shape[2]
    img_local, latent_rows = latents.shape[0], latents.shape[1]
    groups, shards = lax.axis_size("dp"), lax.axis_size("fsdp")
    me, shard = lax.axis_index("dp"), lax.axis_index("fsdp")
    per_sequence = media_refs.shape[1]
    slot_count = media_refs.shape[0] * per_sequence // groups
    capacity = (slot_count + groups - 1) // groups
    tokens = seq_local * window
    gate_scale = jnp.tanh(branch_gate)

    half = groups // 2
    chunks = 2 if head_local % 2 == 0 else 1
    place = jnp.stack([me, shard])

    far_pos = swap(media_pos, "dp", half)
    text_blocks = gather_blocks(text_states.reshape(tokens, feat_local), "fsdp")
    outgoing = outgoing_pairs(media_refs, owner_map, latents, latent_weight, groups, capacity, chunks)
    arrived = []
    for chunk in range(chunks):
        received = {o: swap(outgoing[chunk][o], "dp", o) for o in range(half - 1, 0, -1)}
        arrived.append([outgoing[chunk][0]] + [received[o] for o in range(1, half)])

    normed = norm_rows(place, norm_gain, norm_bias, text_blocks)
    queries = jnp.dot(normed, query_weight.reshape(model_width, head_local * head_size), preferred_element_type=F32)
    queries = (queries * head_size ** (-0.5)).astype(BF16)
    far_queries = swap(queries, "dp", half)

    tables = (queries, media_pos, far_pos, media_refs, owner_map)
    queries, media_pos, far_pos, media_refs, owner_map = lax.optimization_barrier(tables)

    def slots_of(group, positions):
        refs = lax.dynamic_slice_in_dim(media_refs, group * seq_local, seq_local, 0).reshape(slot_count)
        present = refs >= 0
        lookup = jnp.maximum(refs, 0)[:, None] == jnp.arange(owner_map.shape[0], dtype=jnp.int32)
        source = jnp.sum(jnp.where(lookup, owner_map, 0), axis=-1) // img_local
        position = jnp.arange(slot_count, dtype=jnp.int32)
        earlier = (source[:, None] == source[None, :]) & present[None, :] & (position[None, :] < position[:, None])
        slot_of = (source ^ group) * capacity + jnp.sum(earlier.astype(jnp.int32), axis=-1)
        named = positions[:, :, None] == jnp.arange(per_sequence, dtype=jnp.int32)
        slots = jnp.sum(jnp.where(named, slot_of.reshape(seq_local, 1, per_sequence), 0), axis=-1)
        return jnp.where(positions >= 0, slots, -1).reshape(tokens, 1)

    own_slots = slots_of(me, media_pos)
    far_slots = slots_of(me ^ half, far_pos)

    share = tokens // shards
    cols = model_width // groups
    cot = cotangent.reshape(tokens, feat_local)
    pieces = []
    for j in range(shards):
        piece = lax.dynamic_slice(cot, ((shard ^ j) * share, 0), (share, feat_local))
        pieces.append(swap(piece, "fsdp", j) if j else piece)
    pieces, queries = lax.optimization_barrier((pieces, queries))
    share_rows = jnp.zeros((shards, share, feat_local), BF16)
    for j in range(shards):
        share_rows = lax.dynamic_update_slice(share_rows, pieces[j][None], (shard ^ j, 0, 0))
    share_rows = share_rows.reshape(shards, share, feat_local // cols, cols).transpose(0, 2, 1, 3)
    share_rows = lax.all_to_all(share_rows.reshape(groups, share, cols), "dp", 0, 0, tiled=True)
    cot_blocks = gather_blocks(share_rows, "fsdp")
    cot_rows = jnp.zeros((groups, shards, share, cols), BF16)
    for j, block in enumerate(cot_blocks):
        cot_rows = lax.dynamic_update_slice(cot_rows, block[:, None], (0, shard ^ j, 0, 0))
    cot_rows = cot_rows.reshape(groups * tokens, cols)

    contexts, out_grad = [], []
    for chunk in range(chunks):
        partial = attend(own_slots, far_slots, queries, far_queries, arrived[chunk], chunk, latent_rows)
        other = swap(partial, "dp", half)
        context = join(partial, other)
        contexts.append(context)
        gathered = {0: context}
        for o in range(half - 2, 0, -2):
            gathered[o] = swap(context, "dp", o)
        gathered[1] = swap(context, "dp", 1)
        for o in range(half - 2, 0, -2):
            gathered[o + 1] = swap(gathered[o], "dp", 1)
        group_contexts = [gathered[o] for o in range(half)]
        out_grad = [grad_part(place, gate_scale, cot_rows, group_contexts, out_grad)]
    out_grad = out_grad[0]

    weight_rows = output_weight.reshape(head_local * head_size, model_width)
    blocks = dict(enumerate(update_terms(place, contexts, weight_rows, shards)))
    step = 1
    while step < shards:
        kept = {}
        for j in blocks:
            if not j & step:
                received = swap(blocks[j | step].astype(BF16), "fsdp", step)
                kept[j] = blocks[j].astype(F32) + received.astype(F32)
        blocks = kept
        step *= 2
    layer_out = (text_states.reshape(tokens, feat_local).astype(F32) + gate_scale[0] * blocks[0]).astype(BF16)
    return (
        layer_out.reshape(seq_local, window, feat_local),
        out_grad.reshape(head_local, head_size, cols),
    )


def solution(mesh):
    in_specs = (
        P("dp", None, "fsdp"),
        P("dp", None, "fsdp"),
        P(),
        P(),
        P(),
        P(None, "fsdp", None),
        P(None, "fsdp", None),
        P("fsdp", None, None),
        P("dp", None, None),
        P(),
        P("dp", None),
        P(),
    )
    out_specs = (P("dp", None, "fsdp"), P("fsdp", None, "dp"))

    return jax.shard_map(body, mesh=mesh, in_specs=in_specs, out_specs=out_specs, check_vma=False)
```
